32 devices in a mesh: beam: 8 (over y, x, core), grp: 4 (over z).
Axes of the slice: x: 2, y: 2, z: 4, core: 2. Of those that a mesh axis runs over, the one named last changes fastest.
Arguments:
- beam_data: bfloat16 [2, 4096, 256], P(None, 'beam', 'grp'), may hold values from -6 to 6
- window_count: int32 [32], P(('beam', 'grp')), may hold values from 1 to 8
- slot_owner: int32 [32, 8, 1], P(('beam', 'grp')), may hold values from 0 to 7; in each aligned block of 8 rows (0 to 7, 8 to 15, ..., all dimensions but the last counted through in order) at most 2 rows name the same one
- slot_window: int32 [32, 8], P(('beam', 'grp')), may hold values from 0 to 3
- grid_index: int32 [32, 4096], P(('beam', 'grp')), may hold values from 0 to 4095
Outputs:
- spectrum: float32 [32, 4096], P(('beam', 'grp'))
The draws below stay inside these ranges and needn't reach their ends.
Inputs may be any that keep to these rules, and one draw needn't show every extreme that they name: a user's slots 0 to window_count - 1 are live. `slot_owner`: among the 8 slots of the users of one device no owner is named more than 2 times, a bound that some block reaches.
All inputs are finite; a program needn't handle non-finite values.
Results may differ from the reference program's by a relative error of at most 0.0003.
Values may be sent and summed in bfloat16 or wider, within the bound.
A program may use at most 64 MiB of HBM per device.

```python
import math
import jax
import jax.numpy as jnp
import numpy as np
from jax import lax

WIN_BEAMS = 128
NOISE_DIM = 64
WIN_DEV = 4
SNAPS = 256
USER_DEV = 1
SLOTS = 8
GRID = 4096
OVERSAMPLE = 32
ITERS = 8
BEAMS = 4096
USERS = 32
CAP = 2
N_BEAM = 8


def with_ends(drawn, rng, low, largest):
    longest = drawn.shape.index(max(drawn.shape))
    spots = []
    for shift in (0, 1):
        where = [jax.random.randint(jax.random.fold_in(rng, axis), (), 0, length) for axis, length in enumerate(drawn.shape)]
        where[longest] = (where[longest] + shift) % drawn.shape[longest]
        spots.append(tuple(where))
    return drawn.at[spots[0]].set(low).at[spots[1]].set(largest)


def steps_of(own_key, extent, split, smallest, top_value):
    def one(axis_at, parts):
        heights = jax.random.uniform(jax.random.fold_in(jax.random.fold_in(own_key, 6), axis_at), (parts,), jnp.float32, smallest / len(split), top_value / len(split))
        return jnp.repeat(jnp.exp(heights), extent[axis_at] // parts).reshape((-1,) + (1,) * (len(extent) - axis_at - 1))

    gain = one(*split[0])
    for cut in split[1:]:
        gain = gain * one(*cut)
    return gain


def assign_block(own_key, own, number, rows, count, top, limit, skew):
    ranking = jax.random.permutation(own_key, count)
    crowded, common = shares(count, rows * top, limit, skew, True), shares(count, rows * top, limit, skew, False)
    places = jnp.arange(count)

    def named(tallies, offset_by):
        used = int((tallies > 0).sum())
        fixed = max(1, used // 4)
        moved = fixed + (places - fixed + offset_by * (used - fixed)) % max(1, count - fixed)
        return jnp.zeros((count,), jnp.int32).at[ranking[jnp.where(places < fixed, places, moved)]].set(jnp.asarray(tallies, jnp.int32))

    tallies = jnp.where(number % 4 == 0, named(crowded, number // 4), named(common, number - number // 4 - 1))
    mixed = jax.random.permutation(jax.random.fold_in(own, 3), count)
    donor, sink = mixed[0:count // 2 * 2:2], mixed[1:count // 2 * 2:2]
    room = jnp.minimum(tallies[donor] - 1, limit - tallies[sink]) // 2
    room = jnp.where((donor == ranking[0]) | (sink == ranking[0]) | (tallies[sink] == 0), 0, jnp.maximum(room, 0))
    moved = jax.random.randint(jax.random.fold_in(own, 4), (count // 2,), 0, 1 << 20) % (room + 1)
    tallies = tallies.at[donor].add(-moved).at[sink].add(moved)
    items = jnp.searchsorted(jnp.cumsum(tallies), jnp.arange(rows * top), side="right").astype(jnp.int32)
    grid = items.reshape(top, rows).T
    grid = grid[jax.random.permutation(jax.random.fold_in(own, 1), rows)]
    offset_by = jax.random.randint(jax.random.fold_in(own, 2), (rows, 1), 0, top)
    return jnp.take_along_axis(grid, (jnp.arange(top)[None, :] + offset_by) % top, axis=1)


def shares(count, total, bound, slope, full):
    portions = [(1 << 20) // math.isqrt(standing ** slope) + 1 for standing in range(1, count + 1)]
    largest = bound if full else min(bound, max(-(-total // count), total * portions[0] // sum(portions)))
    least = 1 if total - largest >= count - 1 else 0
    given, spare = [largest] + [least] * (count - 1), total - largest - least * (count - 1)
    while spare > 0:
        movable = [i for i in range(1, count) if given[i] < largest] or [i for i in range(1, count) if given[i] < bound]
        mass, remaining = sum([portions[i] for i in movable]), spare
        for i in movable:
            more = min(bound - given[i], max(1, remaining * portions[i] // mass), spare)
            given[i] = given[i] + more
            spare = spare - more
    return np.array(given)


def centred(stream_key, extent, spread, limit, split=(), kind=jnp.bfloat16):
    loudness = steps_of(stream_key, extent, split, -0.22, 0.18) if split else 1.0
    values = jax.random.normal(stream_key, extent, jnp.float32) * spread * loudness
    return jnp.minimum(jnp.maximum(values, -limit), limit).astype(kind)


def setup_inputs(seed: int = 0) -> dict:
    key_list = jax.random.split(jax.random.key(seed), 6)
    beam_data = centred(key_list[0], (2, BEAMS, SNAPS), 1.0, 6.0, ((1, 8), (2, 4)))
    window_count = with_ends(jax.random.randint(key_list[1], (USERS,), 1, SLOTS + 1), jax.random.fold_in(key_list[1], 1), 1, SLOTS).astype(jnp.int32)
    slot_owner_keys = jax.random.split(jax.random.fold_in(key_list[2], 1), USERS * SLOTS // (USER_DEV * SLOTS))
    slot_owner_turns = jax.random.permutation(jax.random.fold_in(key_list[2], 3), USERS * SLOTS // (USER_DEV * SLOTS))
    slot_owner = jax.vmap(lambda own, number: assign_block(jax.random.fold_in(key_list[2], 2), own, number, USER_DEV * SLOTS, N_BEAM, 1, CAP, 2))(slot_owner_keys, slot_owner_turns).reshape((USERS, SLOTS, 1))
    slot_window = with_ends(jax.random.randint(key_list[3], (USERS, SLOTS), 0, WIN_DEV), jax.random.fold_in(key_list[3], 1), 0, WIN_DEV - 1).astype(jnp.int32)
    grid_index = with_ends(jax.random.randint(key_list[4], (USERS, GRID), 0, WIN_BEAMS * OVERSAMPLE), jax.random.fold_in(key_list[4], 1), 0, (WIN_BEAMS * OVERSAMPLE) - 1).astype(jnp.int32)
    return {"beam_data": beam_data, "window_count": window_count, "slot_owner": slot_owner, "slot_window": slot_window, "grid_index": grid_index}


highest = lax.Precision.HIGHEST
shift_factor = 1.05
spectral_floor = 0.05

def orthonormal(image_block):
    gram_matrix = jnp.dot(image_block.T.astype(jnp.float32), image_block.astype(jnp.float32), precision=highest, preferred_element_type=jnp.float32)
    lower_factor = jnp.linalg.cholesky(gram_matrix)
    return jax.scipy.linalg.solve_triangular(lower_factor, image_block.T, lower=True).T

def steering(grid_row, beams_total):
    position = (grid_row.astype(jnp.float32) + 0.5) / OVERSAMPLE
    offset = position[..., None] - jnp.arange(WIN_BEAMS, dtype=jnp.float32)
    turned = jnp.pi * offset
    magnitude = jnp.sin(turned) / (beams_total * jnp.sin(turned / beams_total))
    phase_angle = turned * ((beams_total - 1) / beams_total)
    return jnp.concatenate([magnitude * jnp.cos(phase_angle), magnitude * jnp.sin(phase_angle)], axis=-1)

def reference(beam_data, window_count, slot_owner, slot_window, grid_index):
    windows_all = BEAMS // WIN_BEAMS
    window_view = beam_data.astype(jnp.float32).reshape(2, windows_all, WIN_BEAMS, SNAPS)

    def window_gram(window_pair):
        real_part, imag_part = window_pair
        same_part = jnp.dot(real_part.astype(jnp.float32), real_part.T.astype(jnp.float32), precision=highest, preferred_element_type=jnp.float32)
        same_part = same_part + jnp.dot(imag_part.astype(jnp.float32), imag_part.T.astype(jnp.float32), precision=highest, preferred_element_type=jnp.float32)
        cross_part = jnp.dot(imag_part.astype(jnp.float32), real_part.T.astype(jnp.float32), precision=highest, preferred_element_type=jnp.float32)
        return (same_part, cross_part)
    grams_same, grams_cross = lax.map(window_gram, (window_view[0], window_view[1]))
    window = (slot_owner[:, :, 0] * WIN_DEV + slot_window).astype(jnp.int32)

    def per_user(user_item):
        count_live, window_row, grid_row = user_item
        live_mask = (jnp.arange(SLOTS, dtype=jnp.int32) < count_live).astype(jnp.float32)
        real_sum = jnp.einsum('k,kij->ij', live_mask, grams_same[window_row], precision=highest)
        cross_sum = jnp.einsum('k,kij->ij', live_mask, grams_cross[window_row], precision=highest)
        imag_sum = cross_sum - cross_sum.T
        inverse_count = 1.0 / (count_live.astype(jnp.float32) * SNAPS)
        covariance = jnp.concatenate([jnp.concatenate([real_sum, -imag_sum], axis=1), jnp.concatenate([imag_sum, real_sum], axis=1)], axis=0) * inverse_count
        square = jnp.dot(covariance.astype(jnp.float32), covariance.astype(jnp.float32), precision=highest, preferred_element_type=jnp.float32)
        fourth = jnp.dot(square.astype(jnp.float32), square.astype(jnp.float32), precision=highest, preferred_element_type=jnp.float32)
        shift_value = shift_factor * jnp.sqrt(jnp.sqrt(jnp.sqrt(jnp.sum(fourth * fourth))))
        shifted = shift_value * jnp.eye(2 * WIN_BEAMS, dtype=jnp.float32) - covariance
        start_block = jnp.concatenate([shifted[:, :NOISE_DIM], shifted[:, WIN_BEAMS:WIN_BEAMS + NOISE_DIM]], axis=1)
        noise_basis = orthonormal(start_block)
        for sweep in range(ITERS - 1):
            noise_basis = orthonormal(jnp.dot(shifted.astype(jnp.float32), noise_basis.astype(jnp.float32), precision=highest, preferred_element_type=jnp.float32))
        steering_rows = steering(grid_row, BEAMS)
        projected = jnp.dot(steering_rows.astype(jnp.float32), noise_basis.astype(jnp.float32), precision=highest, preferred_element_type=jnp.float32)
        leakage = lax.optimization_barrier(jnp.sum(projected * projected, axis=-1)) / lax.optimization_barrier(jnp.sum(steering_rows * steering_rows, axis=-1))
        return 1.0 / (leakage + spectral_floor)
    return lax.map(per_user, (window_count, window, grid_index))
```

```python
import functools
import math

import jax
import jax.numpy as jnp
from jax import lax
from jax.experimental import pallas as pl
from jax.experimental.pallas import tpu as pltpu
from jax.sharding import PartitionSpec as P

WIN_BEAMS = 128
NOISE_DIM = 64
SNAPS = 256
OVERSAMPLE = 32
ITERS = 8

MESH = pl.DeviceIdType.MESH
highest = lax.Precision.HIGHEST
shift_factor = 1.05
spectral_floor = 0.05
CHUNK = 512
FAST_LOW = 1.0 / 64
FAST_STEPS = 8


def cubic_schedule(low, steps):
    pairs = []
    for _ in range(steps):
        form = 1.0 + low + low * low
        scale = 3.0 * math.sqrt(3.0) / (2.0 * form**1.5)
        pairs.append((form * scale, scale))
        low = min((low + low * low) * scale, 1.0)
    return pairs


def dot(left, right):
    return jnp.dot(left, right, precision=highest, preferred_element_type=jnp.float32)


def dot_tn(left, right):
    return lax.dot_general(
        left,
        right,
        (((0,), (0,)), ((), ())),
        precision=highest,
        preferred_element_type=jnp.float32,
    )


def dot_nt(left, right):
    return lax.dot_general(
        left, right, (((1,), (1,)), ((), ())), preferred_element_type=jnp.float32
    )


def exchange_kernel(
    n_beam,
    n_grp,
    users,
    windows,
    x_ref,
    weight_ref,
    out_ref,
    held,
    weights_in,
    outgoing,
    incoming,
    x_send,
    x_recv,
    w_send,
    w_recv,
    o_send,
    o_recv,
):
    beam = lax.axis_index("beam")
    grp = lax.axis_index("grp")
    width = WIN_BEAMS

    barrier = pltpu.get_barrier_semaphore()
    for j in range(1, n_grp):
        pl.semaphore_signal(
            barrier, inc=1, device_id=(beam, lax.rem(grp + j, n_grp)), device_id_type=MESH
        )
    for j in range(1, n_beam):
        pl.semaphore_signal(
            barrier, inc=1, device_id=(lax.rem(beam + j, n_beam), grp), device_id_type=MESH
        )
    pl.semaphore_wait(barrier, n_grp + n_beam - 2)

    x_copies = []
    for j in range(1, n_grp):
        copy = pltpu.make_async_remote_copy(
            src_ref=x_ref,
            dst_ref=held.at[j - 1],
            send_sem=x_send.at[j - 1],
            recv_sem=x_recv.at[j - 1],
            device_id=(beam, lax.rem(grp + j, n_grp)),
            device_id_type=MESH,
        )
        copy.start()
        x_copies.append(copy)
    w_copies = []
    for j in range(1, n_beam):
        owner = lax.rem(beam + j, n_beam)
        copy = pltpu.make_async_remote_copy(
            src_ref=weight_ref.at[owner],
            dst_ref=weights_in.at[j - 1],
            send_sem=w_send.at[j - 1],
            recv_sem=w_recv.at[j - 1],
            device_id=(owner, grp),
            device_id_type=MESH,
        )
        copy.start()
        w_copies.append(copy)

    row = lax.broadcasted_iota(jnp.int32, (width, width), 0)
    col = lax.broadcasted_iota(jnp.int32, (width, width), 1)
    lanes = x_ref.shape[1]
    from_lane = lax.broadcasted_iota(jnp.int32, (lanes, lanes), 0)
    to_lane = lax.broadcasted_iota(jnp.int32, (lanes, lanes), 1)
    turn = jnp.where(
        from_lane == to_lane + lanes // 2, -1.0, jnp.where(to_lane == from_lane + lanes // 2, 1.0, 0.0)
    ).astype(jnp.bfloat16)
    same = [None] * windows
    cross = [None] * windows
    for j in range(n_grp):
        if j > 0:
            x_copies[j - 1].wait_recv()
        source = x_ref if j == 0 else held.at[j - 1]
        for w in range(windows):
            piece = source[w * width : (w + 1) * width, :]
            turned = jnp.dot(piece, turn, preferred_element_type=jnp.float32).astype(jnp.bfloat16)
            part_same = dot_nt(piece, piece)
            part_cross = dot_nt(piece, turned)
            same[w] = part_same if j == 0 else same[w] + part_same
            cross[w] = part_cross if j == 0 else cross[w] + part_cross
    packed = [jnp.where(col >= row, same[w], cross[w]) for w in range(windows)]

    def mixed(weights):
        totals = []
        for u in range(users):
            total = packed[0] * weights[u, 0:1, :]
            for w in range(1, windows):
                total = total + packed[w] * weights[u, w : w + 1, :]
            totals.append(total)
        return totals

    o_copies = []
    for j in range(1, n_beam):
        w_copies[j - 1].wait_recv()
        totals = mixed(weights_in[j - 1])
        for u in range(users):
            outgoing[j - 1, u] = totals[u]
    for j in range(1, n_beam):
        copy = pltpu.make_async_remote_copy(
            src_ref=outgoing.at[j - 1],
            dst_ref=incoming.at[j - 1],
            send_sem=o_send.at[j - 1],
            recv_sem=o_recv.at[j - 1],
            device_id=(lax.rem(beam + n_beam - j, n_beam), grp),
            device_id_type=MESH,
        )
        copy.start()
        o_copies.append(copy)
    totals = mixed(weight_ref[beam])
    for j in range(1, n_beam):
        o_copies[j - 1].wait_recv()
        for u in range(users):
            totals[u] = totals[u] + incoming[j - 1, u]
    for u in range(users):
        out_ref[u] = totals[u]
    for copy in x_copies + w_copies + o_copies:
        copy.wait_send()


def exchange(x_local, weights, n_beam, n_grp):
    rows = x_local.shape[0]
    users, padded = weights.shape[1], weights.shape[2]
    windows = rows // WIN_BEAMS
    sums = (users, WIN_BEAMS, WIN_BEAMS)
    return pl.pallas_call(
        functools.partial(exchange_kernel, n_beam, n_grp, users, windows),
        out_shape=jax.ShapeDtypeStruct(sums, jnp.float32),
        in_specs=[pl.BlockSpec(memory_space=pltpu.VMEM)] * 2,
        out_specs=pl.BlockSpec(memory_space=pltpu.VMEM),
        scratch_shapes=[
            pltpu.VMEM((n_grp - 1,) + x_local.shape, jnp.bfloat16),
            pltpu.VMEM((n_beam - 1, users, padded, WIN_BEAMS), jnp.float32),
            pltpu.VMEM((n_beam - 1,) + sums, jnp.float32),
            pltpu.VMEM((n_beam - 1,) + sums, jnp.float32),
            pltpu.SemaphoreType.DMA((n_grp - 1,)),
            pltpu.SemaphoreType.DMA((n_grp - 1,)),
            pltpu.SemaphoreType.DMA((n_beam - 1,)),
            pltpu.SemaphoreType.DMA((n_beam - 1,)),
            pltpu.SemaphoreType.DMA((n_beam - 1,)),
            pltpu.SemaphoreType.DMA((n_beam - 1,)),
        ],
        compiler_params=pltpu.CompilerParams(collective_id=0, has_side_effects=True),
    )(x_local, weights)


def spectrum_kernel(beams_total, sum_ref, count_ref, grid_ref, out_ref, basis_ref):
    width, dim = WIN_BEAMS, NOISE_DIM
    packed = sum_ref[0]
    flipped = packed.T
    row = lax.broadcasted_iota(jnp.int32, (width, width), 0)
    col = lax.broadcasted_iota(jnp.int32, (width, width), 1)
    count = count_ref[pl.program_id(0)].astype(jnp.float32)
    inverse_count = 1.0 / (jnp.zeros((1, width), jnp.float32) + count * SNAPS)
    real_sum = jnp.where(col >= row, packed, flipped) * inverse_count
    imag_sum = jnp.where(col < row, packed, jnp.where(col > row, -flipped, 0.0)) * inverse_count
    covariance = jnp.concatenate(
        [
            jnp.concatenate([real_sum, -imag_sum], axis=1),
            jnp.concatenate([imag_sum, real_sum], axis=1),
        ],
        axis=0,
    )
    square = dot(covariance, covariance)
    fourth = dot(square, square[:, :width])
    energy = 2.0 * jnp.sum(fourth * fourth, keepdims=True)
    shift_value = shift_factor * jnp.sqrt(jnp.sqrt(jnp.sqrt(energy)))
    row2 = lax.broadcasted_iota(jnp.int32, (2 * width, 2 * width), 0)
    col2 = lax.broadcasted_iota(jnp.int32, (2 * width, 2 * width), 1)
    shifted = jnp.where(row2 == col2, 1.0, 0.0) - covariance * (1.0 / shift_value)

    def chosen(matrix):
        return jnp.concatenate([matrix[:, :dim], matrix[:, width : width + dim]], axis=1)

    eye = jnp.where(row == col, 1.0, 0.0)

    def cubic(block, pairs):
        for a, b in pairs:
            gram = dot_tn(block, block)
            block = dot(block, a * eye - b * gram)
        return block

    second = dot(shifted, shifted)
    power = dot(second, second)
    block = dot(power, chosen(power))
    gram = dot_tn(block, block)
    scale = lax.rsqrt(jnp.sqrt(jnp.sum(gram * gram, keepdims=True)))
    block = cubic(block * scale, cubic_schedule(FAST_LOW, FAST_STEPS))
    basis_ref[...] = block
    miss = dot_tn(block, block) - eye
    well = jnp.sum(miss * miss) < 1e-9

    @pl.when(jnp.logical_not(well))
    def _():
        start = jnp.where(
            (row2 == col2)[:, :width] & (col < dim)[:1], 1.0, 0.0
        ) + jnp.where(row2[:, :width] == col2[:, :width] + (width - dim), 1.0, 0.0) * jnp.where(
            col2[:, :width] >= dim, 1.0, 0.0
        )
        basis_ref[...] = start
        pairs = cubic_schedule(0.0132, 5)

        @pl.loop(0, ITERS // 2)
        def _(_):
            basis_ref[...] = cubic(dot(second, basis_ref[...]), pairs)

        basis_ref[...] = cubic(basis_ref[...], [(1.5, 0.5)] * 4)

    theta = row.astype(jnp.float32) * (math.pi / beams_total)
    weight = basis_ref[:width, :] * jnp.cos(theta) + basis_ref[width:, :] * jnp.sin(theta)
    weight = weight.T
    grid_points = grid_ref.shape[-1]
    chunk = math.gcd(CHUNK, grid_points)
    beam_at = lax.broadcasted_iota(jnp.int32, (width, chunk), 0) * OVERSAMPLE
    for at in range(0, grid_points, chunk):
        offset = (grid_ref[0, :, at : at + chunk] - beam_at).astype(jnp.float32) + 0.5
        angle = offset * (math.pi / (OVERSAMPLE * beams_total))
        sq = angle * angle
        sine = offset * (
            1.0 + sq * (-1.0 / 6 + sq * (1.0 / 120 + sq * (-1.0 / 5040 + sq * (1.0 / 362880))))
        )
        steer = OVERSAMPLE / sine
        projected = dot(weight, steer)
        leakage = jnp.sum(projected * projected, axis=0, keepdims=True) / jnp.sum(
            steer * steer, axis=0, keepdims=True
        )
        out_ref[0, :, at : at + chunk] = 1.0 / (leakage + spectral_floor)


def finish_users(sums, counts, grid_index, beams_total):
    users, points = grid_index.shape
    width = WIN_BEAMS
    out = pl.pallas_call(
        functools.partial(spectrum_kernel, beams_total),
        grid=(users,),
        out_shape=jax.ShapeDtypeStruct((users, 1, points), jnp.float32),
        in_specs=[
            pl.BlockSpec((1, width, width), lambda u: (u, 0, 0)),
            pl.BlockSpec(memory_space=pltpu.SMEM),
            pl.BlockSpec((1, 1, points), lambda u: (u, 0, 0)),
        ],
        out_specs=pl.BlockSpec((1, 1, points), lambda u: (u, 0, 0)),
        scratch_shapes=[pltpu.VMEM((2 * width, 2 * NOISE_DIM), jnp.float32)],
    )(sums, counts, grid_index.reshape(users, 1, points))
    return out.reshape(users, points)


def local(n_beam, n_grp, beam_data, window_count, slot_owner, slot_window, grid_index):
    slot_count = slot_window.shape[1]
    windows = beam_data.shape[1] // WIN_BEAMS
    padded = -(-windows // 8) * 8
    beams_total = beam_data.shape[1] * n_beam
    x_local = jnp.concatenate([beam_data[0], beam_data[1]], axis=-1)
    live = jnp.arange(slot_count, dtype=jnp.int32)[None, :] < window_count[:, None]
    named = jnp.where(live, slot_owner[:, :, 0] * padded + slot_window, -1)
    slots = jnp.arange(n_beam * padded, dtype=jnp.int32).reshape(n_beam, 1, padded)
    hits = (named[None, :, None, :] == slots[..., None]).astype(jnp.float32)
    weights = jnp.broadcast_to(
        jnp.sum(hits, axis=-1)[..., None], (n_beam, window_count.shape[0], padded, WIN_BEAMS)
    )
    sums = exchange(x_local, weights, n_beam, n_grp)
    return finish_users(sums, window_count, grid_index, beams_total)


def solution(mesh):
    placed = (
        P(None, "beam", "grp"),
        P(("beam", "grp")),
        P(("beam", "grp"), None, None),
        P(("beam", "grp"), None),
        P(("beam", "grp"), None),
    )
    return jax.shard_map(
        functools.partial(local, mesh.shape["beam"], mesh.shape["grp"]),
        mesh=mesh,
        in_specs=placed,
        out_specs=P(("beam", "grp"), None),
        check_vma=False,
    )
```

```python
import functools
import math

import jax
import jax.numpy as jnp
from jax import lax
from jax.experimental import pallas as pl
from jax.experimental.pallas import tpu as pltpu
from jax.sharding import PartitionSpec as P

WIN_BEAMS = 128
NOISE_DIM = 64
SNAPS = 256
OVERSAMPLE = 32
ITERS = 8

MESH = pl.DeviceIdType.MESH
highest = lax.Precision.HIGHEST
shift_factor = 1.05
spectral_floor = 0.05
CHUNK = 512
FAST_LOW = 1.0 / 36
FAST_STEPS = 7
FAST_COARSE = 4
FAST_MISS = 3e-8


def cubic_schedule(low, steps):
    pairs = []
    for _ in range(steps):
        form = 1.0 + low + low * low
        scale = 3.0 * math.sqrt(3.0) / (2.0 * form**1.5)
        pairs.append((form * scale, scale))
        low = min((low + low * low) * scale, 1.0)
    return pairs


def dot(left, right):
    return jnp.dot(left, right, precision=highest, preferred_element_type=jnp.float32)


def dot_tn(left, right):
    return lax.dot_general(
        left,
        right,
        (((0,), (0,)), ((), ())),
        precision=highest,
        preferred_element_type=jnp.float32,
    )


def halves(matrix):
    high = matrix.astype(jnp.bfloat16)
    return high, (matrix - high.astype(jnp.float32)).astype(jnp.bfloat16)


def plain(left, right, contract=1):
    return lax.dot_general(
        left,
        right,
        (((contract,), (0,)), ((), ())),
        preferred_element_type=jnp.float32,
    )


def dot3(left, right, contract=1):
    (left_high, left_low), (right_high, right_low) = left, right
    return plain(left_high, right_high, contract) + (
        plain(left_high, right_low, contract) + plain(left_low, right_high, contract)
    )


def dot_nt(left, right):
    return lax.dot_general(
        left, right, (((1,), (1,)), ((), ())), preferred_element_type=jnp.float32
    )


def exchange_kernel(
    n_beam,
    n_grp,
    windows,
    beams_total,
    data_ref,
    count_ref,
    owner_ref,
    window_ref,
    grid_ref,
    out_ref,
    high_ref,
    low_ref,
    norm_ref,
    held,
    weights,
    weights_in,
    outgoing,
    incoming,
    same,
    cross,
    x_send,
    x_recv,
    w_send,
    w_recv,
    o_send,
    o_recv,
):
    beam = lax.axis_index("beam")
    grp = lax.axis_index("grp")
    width = WIN_BEAMS
    users, slots = window_ref.shape
    padded = weights.shape[2]

    barrier = pltpu.get_barrier_semaphore()
    has_right = grp < n_grp - 1
    has_left = grp > 0

    @pl.when(has_right)
    def _():
        pl.semaphore_signal(barrier, inc=1, device_id=(beam, grp + 1), device_id_type=MESH)

    @pl.when(has_left)
    def _():
        pl.semaphore_signal(barrier, inc=1, device_id=(beam, grp - 1), device_id_type=MESH)

    for j in range(1, n_beam):
        pl.semaphore_signal(
            barrier, inc=1, device_id=(lax.rem(beam + j, n_beam), grp), device_id_type=MESH
        )

    held[grp] = jnp.concatenate([data_ref[0], data_ref[1]], axis=1)
    entry = lax.broadcasted_iota(jnp.int32, (n_beam, padded, width), 0) * padded + (
        lax.broadcasted_iota(jnp.int32, (n_beam, padded, width), 1)
    )
    for u in range(users):
        total = jnp.zeros((n_beam, padded, width), jnp.float32)
        for k in range(slots):
            named = owner_ref[u, k] * padded + window_ref[u, k]
            live = (k < count_ref[u]).astype(jnp.float32)
            total = total + jnp.where(entry == named, 1.0, 0.0) * live
        weights[:, u] = total

    pl.semaphore_wait(
        barrier, has_right.astype(jnp.int32) + has_left.astype(jnp.int32) + n_beam - 1
    )

    def hop(way, step, w):
        source = grp - (step - 1) if way == 0 else grp + (step - 1)
        rows = pl.ds(w * width, width)
        return pltpu.make_async_remote_copy(
            src_ref=held.at[source, rows],
            dst_ref=held.at[source, rows],
            send_sem=x_send.at[way, step - 1, w],
            recv_sem=x_recv.at[way, step - 1, w],
            device_id=(beam, grp + 1 if way == 0 else grp - 1),
            device_id_type=MESH,
        )

    def arrival(way, step, w):
        source = grp - step if way == 0 else grp + step
        rows = pl.ds(w * width, width)
        return pltpu.make_async_remote_copy(
            src_ref=held.at[source, rows],
            dst_ref=held.at[source, rows],
            send_sem=x_send.at[way, step - 1, w],
            recv_sem=x_recv.at[way, step - 1, w],
            device_id=(beam, grp - 1 if way == 0 else grp + 1),
            device_id_type=MESH,
        )

    def sends(way, step):
        if way == 0:
            return has_right & (grp >= step - 1)
        return has_left & (grp + step - 1 < n_grp)

    def receives(way, step):
        return grp >= step if way == 0 else grp + step < n_grp

    for way in range(2):

        @pl.when(sends(way, 1))
        def _():
            for w in range(windows):
                hop(way, 1, w).start()

    w_copies = []
    for j in range(1, n_beam):
        owner = lax.rem(beam + j, n_beam)
        copy = pltpu.make_async_remote_copy(
            src_ref=weights.at[owner],
            dst_ref=weights_in.at[j - 1],
            send_sem=w_send.at[j - 1],
            recv_sem=w_recv.at[j - 1],
            device_id=(owner, grp),
            device_id_type=MESH,
        )
        copy.start()
        w_copies.append(copy)

    row = lax.broadcasted_iota(jnp.int32, (width, width), 0)
    col = lax.broadcasted_iota(jnp.int32, (width, width), 1)
    lanes = held.shape[2]
    from_lane = lax.broadcasted_iota(jnp.int32, (lanes, lanes), 0)
    to_lane = lax.broadcasted_iota(jnp.int32, (lanes, lanes), 1)
    turn = jnp.where(
        from_lane == to_lane + lanes // 2, -1.0, jnp.where(to_lane == from_lane + lanes // 2, 1.0, 0.0)
    ).astype(jnp.bfloat16)

    def grams(source, w):
        piece = held[source, w * width : (w + 1) * width, :]
        turned = plain(piece, turn).astype(jnp.bfloat16)
        return dot_nt(piece, piece), dot_nt(piece, turned)

    for w in range(windows):
        same[w], cross[w] = grams(grp, w)
    for step in range(1, n_grp):
        for w in range(windows):
            for way in range(2):

                @pl.when(receives(way, step))
                def _():
                    arrival(way, step, w).wait_recv()

                if step < n_grp - 1:

                    @pl.when(sends(way, step + 1))
                    def _():
                        hop(way, step + 1, w).start()

        for way in range(2):

            @pl.when(receives(way, step))
            def _():
                source = grp - step if way == 0 else grp + step
                for w in range(windows):
                    more_same, more_cross = grams(source, w)
                    same[w] += more_same
                    cross[w] += more_cross

    for w in range(windows):
        same[w] = jnp.where(col >= row, same[w], cross[w])

    def mixed(shares, u):
        total = same[0] * shares[u, 0:1, :]
        for w in range(1, windows):
            total = total + same[w] * shares[u, w : w + 1, :]
        return total

    o_copies = []
    for j in range(1, n_beam):
        o_copies.append(
            pltpu.make_async_remote_copy(
                src_ref=outgoing.at[j - 1],
                dst_ref=incoming.at[j - 1],
                send_sem=o_send.at[j - 1],
                recv_sem=o_recv.at[j - 1],
                device_id=(lax.rem(beam + n_beam - j, n_beam), grp),
                device_id_type=MESH,
            )
        )
    for j in range(1, n_beam):
        w_copies[j - 1].wait_recv()
        for u in range(users):
            outgoing[j - 1, u] = mixed(weights_in[j - 1], u)
        if j > 1:
            o_copies[j - 2].start()
    for u in range(users):
        out_ref[u] = mixed(weights[beam], u)
    o_copies[-1].start()

    points = grid_ref.shape[-1]
    chunk = math.gcd(CHUNK, points)
    beam_at = lax.broadcasted_iota(jnp.int32, (width, chunk), 0) * OVERSAMPLE
    for u in range(users):

        @pl.loop(0, points // chunk)
        def _(at):
            span = pl.ds(pl.multiple_of(at * chunk, chunk), chunk)
            offset = (grid_ref[u, :, span] - beam_at).astype(jnp.float32) + 0.5
            angle = offset * (math.pi / (OVERSAMPLE * beams_total))
            sq = angle * angle
            sine = offset * (
                1.0 + sq * (-1.0 / 6 + sq * (1.0 / 120 + sq * (-1.0 / 5040 + sq * (1.0 / 362880))))
            )
            steer = OVERSAMPLE / sine
            high_ref[u, :, span], low_ref[u, :, span] = halves(steer)
            norm_ref[u, :, span] = jnp.sum(steer * steer, axis=0, keepdims=True)

    for j in range(1, n_beam):
        o_copies[j - 1].wait_recv()
        for u in range(users):
            out_ref[u] += incoming[j - 1, u]
    for copy in w_copies + o_copies:
        copy.wait_send()
    for way in range(2):
        for step in range(1, n_grp):

            @pl.when(sends(way, step))
            def _():
                for w in range(windows):
                    hop(way, step, w).wait_send()


def exchange(beam_data, counts, owners, slot_window, grid_index, n_beam, n_grp):
    rows = beam_data.shape[1]
    windows = rows // WIN_BEAMS
    padded = -(-windows // 8) * 8
    users, points = grid_index.shape[0], grid_index.shape[2]
    width = WIN_BEAMS
    sums = (users, width, width)
    shares = (users, padded, width)
    vmem = pl.BlockSpec(memory_space=pltpu.VMEM)
    smem = pl.BlockSpec(memory_space=pltpu.SMEM)
    return pl.pallas_call(
        functools.partial(exchange_kernel, n_beam, n_grp, windows, rows * n_beam),
        out_shape=[
            jax.ShapeDtypeStruct(sums, jnp.float32),
            jax.ShapeDtypeStruct((users, width, points), jnp.bfloat16),
            jax.ShapeDtypeStruct((users, width, points), jnp.bfloat16),
            jax.ShapeDtypeStruct((users, 1, points), jnp.float32),
        ],
        in_specs=[vmem, smem, smem, smem, vmem],
        out_specs=[vmem] * 4,
        scratch_shapes=[
            pltpu.VMEM((n_grp, rows, 2 * beam_data.shape[2]), jnp.bfloat16),
            pltpu.VMEM((n_beam,) + shares, jnp.float32),
            pltpu.VMEM((n_beam - 1,) + shares, jnp.float32),
            pltpu.VMEM((n_beam - 1,) + sums, jnp.float32),
            pltpu.VMEM((n_beam - 1,) + sums, jnp.float32),
            pltpu.VMEM((windows, width, width), jnp.float32),
            pltpu.VMEM((windows, width, width), jnp.float32),
            pltpu.SemaphoreType.DMA((2, n_grp - 1, windows)),
            pltpu.SemaphoreType.DMA((2, n_grp - 1, windows)),
            pltpu.SemaphoreType.DMA((n_beam - 1,)),
            pltpu.SemaphoreType.DMA((n_beam - 1,)),
            pltpu.SemaphoreType.DMA((n_beam - 1,)),
            pltpu.SemaphoreType.DMA((n_beam - 1,)),
        ],
        compiler_params=pltpu.CompilerParams(collective_id=0, has_side_effects=True),
    )(beam_data, counts, owners, slot_window, grid_index)


def spectrum_kernel(
    beams_total, sum_ref, count_ref, high_ref, low_ref, norm_ref, out_ref, basis_ref
):
    width, dim = WIN_BEAMS, NOISE_DIM
    packed = sum_ref[0]
    flipped = packed.T
    row = lax.broadcasted_iota(jnp.int32, (width, width), 0)
    col = lax.broadcasted_iota(jnp.int32, (width, width), 1)
    count = count_ref[pl.program_id(0)].astype(jnp.float32)
    inverse_count = 1.0 / (jnp.zeros((1, width), jnp.float32) + count * SNAPS)
    real_sum = jnp.where(col >= row, packed, flipped) * inverse_count
    imag_sum = jnp.where(col < row, packed, jnp.where(col > row, -flipped, 0.0)) * inverse_count
    covariance = jnp.concatenate(
        [
            jnp.concatenate([real_sum, -imag_sum], axis=1),
            jnp.concatenate([imag_sum, real_sum], axis=1),
        ],
        axis=0,
    )
    parts = halves(covariance)
    square = halves(dot3(parts, parts))
    fourth = dot3(square, [half[:, :width] for half in square])
    energy = 2.0 * jnp.sum(fourth * fourth, keepdims=True)
    shift_value = shift_factor * jnp.sqrt(jnp.sqrt(jnp.sqrt(energy)))
    row2 = lax.broadcasted_iota(jnp.int32, (2 * width, 2 * width), 0)
    col2 = lax.broadcasted_iota(jnp.int32, (2 * width, 2 * width), 1)
    shifted = jnp.where(row2 == col2, 1.0, 0.0) - covariance * (1.0 / shift_value)

    def chosen(matrix):
        return jnp.concatenate([matrix[:, :dim], matrix[:, width : width + dim]], axis=1)

    eye = jnp.where(row == col, 1.0, 0.0)

    def cubic(block, pairs):
        for a, b in pairs:
            gram = dot_tn(block, block)
            block = dot(block, a * eye - b * gram)
        return block

    parts = halves(shifted)
    second = halves(dot3(parts, parts))
    power = dot3(second, second)
    block = dot3(halves(power), halves(chosen(power)))
    parts = halves(block)
    gram = dot3(parts, parts, 0)
    scale = 2.0**0.25 * lax.rsqrt(jnp.sqrt(jnp.sum(gram * gram, keepdims=True)))
    block, gram = block * scale, gram * (scale * scale)
    for step, (a, b) in enumerate(cubic_schedule(FAST_LOW, FAST_STEPS)):
        parts = halves(block)
        if step >= FAST_COARSE:
            gram = dot3(parts, parts, 0)
        elif step > 0:
            gram = plain(parts[0], parts[0], 0)
        block = a * block - b * dot3(parts, halves(gram))
    basis_ref[...] = block
    parts = halves(block)
    miss = dot3(parts, parts, 0) - eye
    well = jnp.sum(miss * miss) < FAST_MISS

    @pl.when(jnp.logical_not(well))
    def _():
        start = jnp.where(
            (row2 == col2)[:, :width] & (col < dim)[:1], 1.0, 0.0
        ) + jnp.where(row2[:, :width] == col2[:, :width] + (width - dim), 1.0, 0.0) * jnp.where(
            col2[:, :width] >= dim, 1.0, 0.0
        )
        basis_ref[...] = start
        second = dot(shifted, shifted)
        pairs = cubic_schedule(0.0132, 5)

        @pl.loop(0, ITERS // 2)
        def _(_):
            basis_ref[...] = cubic(dot(second, basis_ref[...]), pairs)

        basis_ref[...] = cubic(basis_ref[...], [(1.5, 0.5)] * 4)

    theta = row.astype(jnp.float32) * (math.pi / beams_total)
    weight = basis_ref[:width, :] * jnp.cos(theta) + basis_ref[width:, :] * jnp.sin(theta)
    weight = weight.T
    weight = halves(weight)
    points = norm_ref.shape[-1]
    chunk = math.gcd(CHUNK, points)
    for at in range(0, points, chunk):
        span = slice(at, at + chunk)
        projected = dot3(weight, (high_ref[0, :, span], low_ref[0, :, span]))
        leakage = jnp.sum(projected * projected, axis=0, keepdims=True) / norm_ref[0, :, span]
        out_ref[0, :, span] = 1.0 / (leakage + spectral_floor)


def finish_users(sums, counts, high, low, norm, beams_total):
    users, width, points = high.shape

    def block(*shape):
        return pl.BlockSpec((1,) + shape, lambda u: (u, 0, 0))

    return pl.pallas_call(
        functools.partial(spectrum_kernel, beams_total),
        grid=(users,),
        out_shape=jax.ShapeDtypeStruct((users, 1, points), jnp.float32),
        in_specs=[
            block(width, width),
            pl.BlockSpec(memory_space=pltpu.SMEM),
            block(width, points),
            block(width, points),
            block(1, points),
        ],
        out_specs=block(1, points),
        scratch_shapes=[pltpu.VMEM((2 * width, 2 * NOISE_DIM), jnp.float32)],
    )(sums, counts, high, low, norm).reshape(users, points)


def local(n_beam, n_grp, beam_data, window_count, slot_owner, slot_window, grid_index):
    users, points = grid_index.shape
    sums, high, low, norm = exchange(
        beam_data,
        window_count,
        slot_owner[:, :, 0],
        slot_window,
        grid_index.reshape(users, 1, points),
        n_beam,
        n_grp,
    )
    return finish_users(
        sums, window_count, high, low, norm, beam_data.shape[1] * n_beam
    )


def solution(mesh):
    placed = (
        P(None, "beam", "grp"),
        P(("beam", "grp")),
        P(("beam", "grp"), None, None),
        P(("beam", "grp"), None),
        P(("beam", "grp"), None),
    )
    return jax.shard_map(
        functools.partial(local, mesh.shape["beam"], mesh.shape["grp"]),
        mesh=mesh,
        in_specs=placed,
        out_specs=P(("beam", "grp"), None),
        check_vma=False,
    )
```

```python
import functools
import math

import jax
import jax.numpy as jnp
from jax import lax
from jax.experimental import pallas as pl
from jax.experimental.pallas import tpu as pltpu
from jax.sharding import PartitionSpec as P

WIN_BEAMS = 128
NOISE_DIM = 64
SNAPS = 256
OVERSAMPLE = 32
ITERS = 8

MESH = pl.DeviceIdType.MESH
highest = lax.Precision.HIGHEST
shift_factor = 1.05
spectral_floor = 0.05
CHUNK = 512
FAST_LOW = 1.0 / 36
FAST_STEPS = 7
FAST_COARSE = 4
FAST_MISS = 2e-4


def cubic_schedule(low, steps):
    pairs = []
    for _ in range(steps):
        form = 1.0 + low + low * low
        scale = 3.0 * math.sqrt(3.0) / (2.0 * form**1.5)
        pairs.append((form * scale, scale))
        low = min((low + low * low) * scale, 1.0)
    return pairs


def dot(left, right):
    return jnp.dot(left, right, precision=highest, preferred_element_type=jnp.float32)


def dot_tn(left, right):
    return lax.dot_general(
        left,
        right,
        (((0,), (0,)), ((), ())),
        precision=highest,
        preferred_element_type=jnp.float32,
    )


def halves(matrix):
    high = matrix.astype(jnp.bfloat16)
    return high, (matrix - high.astype(jnp.float32)).astype(jnp.bfloat16)


def plain(left, right, contract=1):
    return lax.dot_general(
        left,
        right,
        (((contract,), (0,)), ((), ())),
        preferred_element_type=jnp.float32,
    )


def dot3(left, right, contract=1):
    (left_high, left_low), (right_high, right_low) = left, right
    return plain(left_high, right_high, contract) + (
        plain(left_high, right_low, contract) + plain(left_low, right_high, contract)
    )


def dot_nt(left, right):
    return lax.dot_general(
        left, right, (((1,), (1,)), ((), ())), preferred_element_type=jnp.float32
    )


def exchange_kernel(
    n_beam,
    n_grp,
    windows,
    beams_total,
    data_ref,
    count_ref,
    owner_ref,
    window_ref,
    grid_ref,
    out_ref,
    high_ref,
    low_ref,
    norm_ref,
    held,
    weights,
    weights_in,
    outgoing,
    incoming,
    same,
    cross,
    high_made,
    low_made,
    store_sem,
    x_send,
    x_recv,
    w_send,
    w_recv,
    o_send,
    o_recv,
):
    beam = lax.axis_index("beam")
    grp = lax.axis_index("grp")
    width = WIN_BEAMS
    users, slots = window_ref.shape
    padded = weights.shape[2]

    barrier = pltpu.get_barrier_semaphore()
    has_right = grp < n_grp - 1
    has_left = grp > 0

    @pl.when(has_right)
    def _():
        pl.semaphore_signal(barrier, inc=1, device_id=(beam, grp + 1), device_id_type=MESH)

    @pl.when(has_left)
    def _():
        pl.semaphore_signal(barrier, inc=1, device_id=(beam, grp - 1), device_id_type=MESH)

    for j in range(1, n_beam):
        pl.semaphore_signal(
            barrier, inc=1, device_id=(lax.rem(beam + j, n_beam), grp), device_id_type=MESH
        )

    for w in range(windows):
        columns = slice(w * width, (w + 1) * width)
        held[grp, w] = jnp.concatenate([data_ref[0, :, columns], data_ref[1, :, columns]], axis=0)
    entry = lax.broadcasted_iota(jnp.int32, (n_beam, padded, width), 0) * padded + (
        lax.broadcasted_iota(jnp.int32, (n_beam, padded, width), 1)
    )
    for u in range(users):
        total = jnp.zeros((n_beam, padded, width), jnp.float32)
        for k in range(slots):
            named = owner_ref[u, k] * padded + window_ref[u, k]
            live = (k < count_ref[u]).astype(jnp.float32)
            total = total + jnp.where(entry == named, 1.0, 0.0) * live
        weights[:, u] = total

    pl.semaphore_wait(
        barrier, has_right.astype(jnp.int32) + has_left.astype(jnp.int32) + n_beam - 1
    )

    def hop(way, step, w):
        source = grp - (step - 1) if way == 0 else grp + (step - 1)
        return pltpu.make_async_remote_copy(
            src_ref=held.at[source, w],
            dst_ref=held.at[source, w],
            send_sem=x_send.at[way, step - 1, w],
            recv_sem=x_recv.at[way, step - 1, w],
            device_id=(beam, grp + 1 if way == 0 else grp - 1),
            device_id_type=MESH,
        )

    def arrival(way, step, w):
        source = grp - step if way == 0 else grp + step
        return pltpu.make_async_remote_copy(
            src_ref=held.at[source, w],
            dst_ref=held.at[source, w],
            send_sem=x_send.at[way, step - 1, w],
            recv_sem=x_recv.at[way, step - 1, w],
            device_id=(beam, grp - 1 if way == 0 else grp + 1),
            device_id_type=MESH,
        )

    def sends(way, step):
        if way == 0:
            return has_right & (grp >= step - 1)
        return has_left & (grp + step - 1 < n_grp)

    def receives(way, step):
        return grp >= step if way == 0 else grp + step < n_grp

    for way in range(2):

        @pl.when(sends(way, 1))
        def _():
            for w in range(windows):
                hop(way, 1, w).start()

    w_copies = []
    for j in range(1, n_beam):
        owner = lax.rem(beam + j, n_beam)
        copy = pltpu.make_async_remote_copy(
            src_ref=weights.at[owner],
            dst_ref=weights_in.at[j - 1],
            send_sem=w_send.at[j - 1],
            recv_sem=w_recv.at[j - 1],
            device_id=(owner, grp),
            device_id_type=MESH,
        )
        copy.start()
        w_copies.append(copy)

    row = lax.broadcasted_iota(jnp.int32, (width, width), 0)
    col = lax.broadcasted_iota(jnp.int32, (width, width), 1)
    half = held.shape[2] // 2

    def grams(source, w):
        piece = held[source, w]
        turned = jnp.concatenate([-piece[half:], piece[:half]], axis=0)
        return plain(piece, piece, 0), plain(piece, turned, 0)

    for w in range(windows):
        same[w], cross[w] = grams(grp, w)
    for step in range(1, n_grp):
        for w in range(windows):
            for way in range(2):

                @pl.when(receives(way, step))
                def _():
                    arrival(way, step, w).wait_recv()

                if step < n_grp - 1:

                    @pl.when(sends(way, step + 1))
                    def _():
                        hop(way, step + 1, w).start()

            for way in range(2):

                @pl.when(receives(way, step))
                def _():
                    source = grp - step if way == 0 else grp + step
                    more_same, more_cross = grams(source, w)
                    same[w] += more_same
                    cross[w] += more_cross

    for w in range(windows):
        same[w] = jnp.where(col >= row, same[w], cross[w])

    def mixed(shares, u):
        total = same[0] * shares[u, 0:1, :]
        for w in range(1, windows):
            total = total + same[w] * shares[u, w : w + 1, :]
        return total

    o_copies = []
    for j in range(1, n_beam):
        o_copies.append(
            pltpu.make_async_remote_copy(
                src_ref=outgoing.at[j - 1],
                dst_ref=incoming.at[j - 1],
                send_sem=o_send.at[j - 1],
                recv_sem=o_recv.at[j - 1],
                device_id=(lax.rem(beam + n_beam - j, n_beam), grp),
                device_id_type=MESH,
            )
        )
    for j in range(1, n_beam):
        w_copies[j - 1].wait_recv()
        for u in range(users):
            outgoing[j - 1, u] = mixed(weights_in[j - 1], u)
        if j > 1:
            o_copies[j - 2].start()
    for u in range(users):
        out_ref[u] = mixed(weights[beam], u)
    o_copies[-1].start()

    points = grid_ref.shape[-1]
    chunk = math.gcd(CHUNK, points)
    beam_at = lax.broadcasted_iota(jnp.int32, (width, chunk), 0) * OVERSAMPLE
    for u in range(users):

        @pl.loop(0, points // chunk)
        def _(at):
            span = pl.ds(pl.multiple_of(at * chunk, chunk), chunk)
            offset = (grid_ref[u, :, span] - beam_at).astype(jnp.float32) + 0.5
            angle = offset * (math.pi / (OVERSAMPLE * beams_total))
            sq = angle * angle
            sine = offset * (
                1.0 + sq * (-1.0 / 6 + sq * (1.0 / 120 + sq * (-1.0 / 5040 + sq * (1.0 / 362880))))
            )
            steer = OVERSAMPLE / sine
            high_made[u, :, span], low_made[u, :, span] = halves(steer)
            norm_ref[u, :, span] = jnp.sum(steer * steer, axis=0, keepdims=True)

    stored = [
        pltpu.make_async_copy(high_made, high_ref, store_sem.at[0]),
        pltpu.make_async_copy(low_made, low_ref, store_sem.at[1]),
    ]
    for copy in stored:
        copy.start()
    for j in range(1, n_beam):
        o_copies[j - 1].wait_recv()
        for u in range(users):
            out_ref[u] += incoming[j - 1, u]
    for copy in w_copies + o_copies:
        copy.wait_send()
    for copy in stored:
        copy.wait()
    for way in range(2):
        for step in range(1, n_grp):

            @pl.when(sends(way, step))
            def _():
                for w in range(windows):
                    hop(way, step, w).wait_send()


def exchange(beam_data, counts, owners, slot_window, grid_index, n_beam, n_grp):
    rows = beam_data.shape[2]
    windows = rows // WIN_BEAMS
    padded = -(-windows // 8) * 8
    users, points = grid_index.shape[0], grid_index.shape[2]
    width = WIN_BEAMS
    sums = (users, width, width)
    shares = (users, padded, width)
    vmem = pl.BlockSpec(memory_space=pltpu.VMEM)
    smem = pl.BlockSpec(memory_space=pltpu.SMEM)
    anywhere = pl.BlockSpec(memory_space=pl.ANY)
    return pl.pallas_call(
        functools.partial(exchange_kernel, n_beam, n_grp, windows, rows * n_beam),
        out_shape=[
            jax.ShapeDtypeStruct(sums, jnp.float32),
            jax.ShapeDtypeStruct((users, width, points), jnp.bfloat16),
            jax.ShapeDtypeStruct((users, width, points), jnp.bfloat16),
            jax.ShapeDtypeStruct((users, 1, points), jnp.float32),
        ],
        in_specs=[vmem, smem, smem, smem, vmem],
        out_specs=[vmem, anywhere, anywhere, vmem],
        scratch_shapes=[
            pltpu.VMEM((n_grp, windows, 2 * beam_data.shape[1], width), jnp.bfloat16),
            pltpu.VMEM((n_beam,) + shares, jnp.float32),
            pltpu.VMEM((n_beam - 1,) + shares, jnp.float32),
            pltpu.VMEM((n_beam - 1,) + sums, jnp.float32),
            pltpu.VMEM((n_beam - 1,) + sums, jnp.float32),
            pltpu.VMEM((windows, width, width), jnp.float32),
            pltpu.VMEM((windows, width, width), jnp.float32),
            pltpu.VMEM((users, width, points), jnp.bfloat16),
            pltpu.VMEM((users, width, points), jnp.bfloat16),
            pltpu.SemaphoreType.DMA((2,)),
            pltpu.SemaphoreType.DMA((2, n_grp - 1, windows)),
            pltpu.SemaphoreType.DMA((2, n_grp - 1, windows)),
            pltpu.SemaphoreType.DMA((n_beam - 1,)),
            pltpu.SemaphoreType.DMA((n_beam - 1,)),
            pltpu.SemaphoreType.DMA((n_beam - 1,)),
            pltpu.SemaphoreType.DMA((n_beam - 1,)),
        ],
        compiler_params=pltpu.CompilerParams(collective_id=0, has_side_effects=True),
    )(beam_data, counts, owners, slot_window, grid_index)


def spectrum_kernel(
    beams_total, sum_ref, count_ref, high_ref, low_ref, norm_ref, out_ref, basis_ref, high, low, load_sem
):
    user = pl.program_id(0)
    loads = [
        pltpu.make_async_copy(high_ref.at[user], high, load_sem.at[0]),
        pltpu.make_async_copy(low_ref.at[user], low, load_sem.at[1]),
    ]
    for copy in loads:
        copy.start()
    width, dim = WIN_BEAMS, NOISE_DIM
    packed = sum_ref[0]
    flipped = packed.T
    row = lax.broadcasted_iota(jnp.int32, (width, width), 0)
    col = lax.broadcasted_iota(jnp.int32, (width, width), 1)
    count = count_ref[user].astype(jnp.float32)
    inverse_count = 1.0 / (jnp.zeros((1, width), jnp.float32) + count * SNAPS)
    real_sum = jnp.where(col >= row, packed, flipped) * inverse_count
    imag_sum = jnp.where(col < row, packed, jnp.where(col > row, -flipped, 0.0)) * inverse_count
    covariance = jnp.concatenate(
        [
            jnp.concatenate([real_sum, -imag_sum], axis=1),
            jnp.concatenate([imag_sum, real_sum], axis=1),
        ],
        axis=0,
    )
    parts = halves(covariance)
    square = halves(dot3(parts, parts))
    fourth = dot3(square, [half[:, :width] for half in square])
    energy = 2.0 * jnp.sum(fourth * fourth, keepdims=True)
    shift_value = shift_factor * jnp.sqrt(jnp.sqrt(jnp.sqrt(energy)))
    row2 = lax.broadcasted_iota(jnp.int32, (2 * width, 2 * width), 0)
    col2 = lax.broadcasted_iota(jnp.int32, (2 * width, 2 * width), 1)
    shifted = jnp.where(row2 == col2, 1.0, 0.0) - covariance * (1.0 / shift_value)

    def chosen(matrix):
        return jnp.concatenate([matrix[:, :dim], matrix[:, width : width + dim]], axis=1)

    eye = jnp.where(row == col, 1.0, 0.0)

    def cubic(block, pairs):
        for a, b in pairs:
            gram = dot_tn(block, block)
            block = dot(block, a * eye - b * gram)
        return block

    parts = halves(shifted)
    second = halves(dot3(parts, parts))
    power = dot3(second, second)
    block = dot3(halves(power), halves(chosen(power)))
    parts = halves(block)
    gram = dot3(parts, parts, 0)
    scale = 2.0**0.25 * lax.rsqrt(jnp.sqrt(jnp.sum(gram * gram, keepdims=True)))
    block, gram = block * scale, gram * (scale * scale)
    for step, (a, b) in enumerate(cubic_schedule(FAST_LOW, FAST_STEPS)):
        parts = halves(block)
        if step >= FAST_COARSE:
            gram = dot3(parts, parts, 0)
        elif step > 0:
            gram = plain(parts[0], parts[0], 0)
        block = a * block - b * dot3(parts, halves(gram))
    miss = gram - eye
    well = jnp.sum(miss * miss) < FAST_MISS

    def put(basis):
        theta = row.astype(jnp.float32) * (math.pi / beams_total)
        weight = basis[:width] * jnp.cos(theta) + basis[width:] * jnp.sin(theta)
        weight = halves(weight.T)
        points = norm_ref.shape[-1]
        chunk = math.gcd(CHUNK, points)
        for at in range(0, points, chunk):
            span = slice(at, at + chunk)
            projected = dot3(weight, (high[:, span], low[:, span]))
            leakage = jnp.sum(projected * projected, axis=0, keepdims=True) / norm_ref[0, :, span]
            out_ref[0, :, span] = 1.0 / (leakage + spectral_floor)

    for copy in loads:
        copy.wait()
    put(block)

    @pl.when(jnp.logical_not(well))
    def _():
        start = jnp.where(
            (row2 == col2)[:, :width] & (col < dim)[:1], 1.0, 0.0
        ) + jnp.where(row2[:, :width] == col2[:, :width] + (width - dim), 1.0, 0.0) * jnp.where(
            col2[:, :width] >= dim, 1.0, 0.0
        )
        basis_ref[...] = start
        second = dot(shifted, shifted)
        pairs = cubic_schedule(0.0132, 5)

        @pl.loop(0, ITERS // 2)
        def _(_):
            basis_ref[...] = cubic(dot(second, basis_ref[...]), pairs)

        basis_ref[...] = cubic(basis_ref[...], [(1.5, 0.5)] * 4)
        put(basis_ref[...])


def finish_users(sums, counts, high, low, norm, beams_total):
    users, width, points = high.shape

    def block(*shape):
        return pl.BlockSpec((1,) + shape, lambda u: (u, 0, 0))

    return pl.pallas_call(
        functools.partial(spectrum_kernel, beams_total),
        grid=(users,),
        out_shape=jax.ShapeDtypeStruct((users, 1, points), jnp.float32),
        in_specs=[
            block(width, width),
            pl.BlockSpec(memory_space=pltpu.SMEM),
            pl.BlockSpec(memory_space=pl.ANY),
            pl.BlockSpec(memory_space=pl.ANY),
            block(1, points),
        ],
        out_specs=block(1, points),
        scratch_shapes=[
            pltpu.VMEM((2 * width, 2 * NOISE_DIM), jnp.float32),
            pltpu.VMEM((width, points), jnp.bfloat16),
            pltpu.VMEM((width, points), jnp.bfloat16),
            pltpu.SemaphoreType.DMA((2,)),
        ],
    )(sums, counts, high, low, norm).reshape(users, points)


def local(n_beam, n_grp, beam_data, window_count, slot_owner, slot_window, grid_index):
    users, points = grid_index.shape
    sums, high, low, norm = exchange(
        jnp.swapaxes(beam_data, 1, 2),
        window_count,
        slot_owner[:, :, 0],
        slot_window,
        grid_index.reshape(users, 1, points),
        n_beam,
        n_grp,
    )
    return finish_users(
        sums, window_count, high, low, norm, beam_data.shape[1] * n_beam
    )


def solution(mesh):
    placed = (
        P(None, "beam", "grp"),
        P(("beam", "grp")),
        P(("beam", "grp"), None, None),
        P(("beam", "grp"), None),
        P(("beam", "grp"), None),
    )
    return jax.shard_map(
        functools.partial(local, mesh.shape["beam"], mesh.shape["grp"]),
        mesh=mesh,
        in_specs=placed,
        out_specs=P(("beam", "grp"), None),
        check_vma=False,
    )
```

```python
import functools
import math

import jax
import jax.numpy as jnp
from jax import lax
from jax.experimental import pallas as pl
from jax.experimental.pallas import tpu as pltpu
from jax.sharding import PartitionSpec as P

WIN_BEAMS = 128
NOISE_DIM = 64
SNAPS = 256
OVERSAMPLE = 32
ITERS = 8

MESH = pl.DeviceIdType.MESH
highest = lax.Precision.HIGHEST
shift_factor = 1.05
spectral_floor = 0.05
CHUNK = 512
FAST_LOW = 1.0 / 36
FAST_STEPS = 7
FAST_COARSE = 4
FAST_MISS = 2e-4


def cubic_schedule(low, steps):
    pairs = []
    for _ in range(steps):
        form = 1.0 + low + low * low
        scale = 3.0 * math.sqrt(3.0) / (2.0 * form**1.5)
        pairs.append((form * scale, scale))
        low = min((low + low * low) * scale, 1.0)
    return pairs


def dot(left, right):
    return jnp.dot(left, right, precision=highest, preferred_element_type=jnp.float32)


def dot_tn(left, right):
    return lax.dot_general(
        left,
        right,
        (((0,), (0,)), ((), ())),
        precision=highest,
        preferred_element_type=jnp.float32,
    )


def halves(matrix):
    high = matrix.astype(jnp.bfloat16)
    return high, (matrix - high.astype(jnp.float32)).astype(jnp.bfloat16)


def plain(left, right, contract=1):
    return lax.dot_general(
        left,
        right,
        (((contract,), (0,)), ((), ())),
        preferred_element_type=jnp.float32,
    )


def dot3(left, right, contract=1):
    (left_high, left_low), (right_high, right_low) = left, right
    return plain(left_high, right_high, contract) + (
        plain(left_high, right_low, contract) + plain(left_low, right_high, contract)
    )


def dot_nt(left, right):
    return lax.dot_general(
        left, right, (((1,), (1,)), ((), ())), preferred_element_type=jnp.float32
    )


def exchange_kernel(
    n_beam,
    n_grp,
    windows,
    beams_total,
    data_ref,
    count_ref,
    owner_ref,
    window_ref,
    grid_ref,
    out_ref,
    high_ref,
    low_ref,
    norm_ref,
    held,
    weights,
    weights_in,
    passing,
    passed,
    outgoing,
    incoming,
    same,
    cross,
    high_made,
    low_made,
    store_sem,
    x_send,
    x_recv,
    w_send,
    w_recv,
    p_send,
    p_recv,
    o_send,
    o_recv,
):
    beam = lax.axis_index("beam")
    grp = lax.axis_index("grp")
    width = WIN_BEAMS
    users, slots = window_ref.shape
    padded = weights.shape[2]

    barrier = pltpu.get_barrier_semaphore()
    has_right = grp < n_grp - 1
    has_left = grp > 0

    @pl.when(has_right)
    def _():
        pl.semaphore_signal(barrier, inc=1, device_id=(beam, grp + 1), device_id_type=MESH)

    @pl.when(has_left)
    def _():
        pl.semaphore_signal(barrier, inc=1, device_id=(beam, grp - 1), device_id_type=MESH)

    for j in range(1, n_beam):
        pl.semaphore_signal(
            barrier, inc=1, device_id=(lax.rem(beam + j, n_beam), grp), device_id_type=MESH
        )

    for w in range(windows):
        columns = slice(w * width, (w + 1) * width)
        held[grp, w] = jnp.concatenate([data_ref[0, :, columns], data_ref[1, :, columns]], axis=0)
    entry = lax.broadcasted_iota(jnp.int32, (n_beam, padded, width), 0) * padded + (
        lax.broadcasted_iota(jnp.int32, (n_beam, padded, width), 1)
    )
    for u in range(users):
        total = jnp.zeros((n_beam, padded, width), jnp.float32)
        for k in range(slots):
            named = owner_ref[u, k] * padded + window_ref[u, k]
            live = (k < count_ref[u]).astype(jnp.float32)
            total = total + jnp.where(entry == named, 1.0, 0.0) * live
        weights[:, u] = total

    pl.semaphore_wait(
        barrier, has_right.astype(jnp.int32) + has_left.astype(jnp.int32) + n_beam - 1
    )

    def hop(way, step, w):
        source = grp - (step - 1) if way == 0 else grp + (step - 1)
        return pltpu.make_async_remote_copy(
            src_ref=held.at[source, w],
            dst_ref=held.at[source, w],
            send_sem=x_send.at[way, step - 1, w],
            recv_sem=x_recv.at[way, step - 1, w],
            device_id=(beam, grp + 1 if way == 0 else grp - 1),
            device_id_type=MESH,
        )

    def arrival(way, step, w):
        source = grp - step if way == 0 else grp + step
        return pltpu.make_async_remote_copy(
            src_ref=held.at[source, w],
            dst_ref=held.at[source, w],
            send_sem=x_send.at[way, step - 1, w],
            recv_sem=x_recv.at[way, step - 1, w],
            device_id=(beam, grp - 1 if way == 0 else grp + 1),
            device_id_type=MESH,
        )

    def sends(way, step):
        if way == 0:
            return has_right & (grp >= step - 1)
        return has_left & (grp + step - 1 < n_grp)

    def receives(way, step):
        return grp >= step if way == 0 else grp + step < n_grp

    for way in range(2):

        @pl.when(sends(way, 1))
        def _():
            for w in range(windows):
                hop(way, 1, w).start()

    w_copies = []
    for j in range(1, n_beam):
        owner = lax.rem(beam + j, n_beam)
        copy = pltpu.make_async_remote_copy(
            src_ref=weights.at[owner],
            dst_ref=weights_in.at[j - 1],
            send_sem=w_send.at[j - 1],
            recv_sem=w_recv.at[j - 1],
            device_id=(owner, grp),
            device_id_type=MESH,
        )
        copy.start()
        w_copies.append(copy)

    row = lax.broadcasted_iota(jnp.int32, (width, width), 0)
    col = lax.broadcasted_iota(jnp.int32, (width, width), 1)
    half = held.shape[2] // 2

    def grams(source, w):
        piece = held[source, w]
        turned = jnp.concatenate([-piece[half:], piece[:half]], axis=0)
        return plain(piece, piece, 0), plain(piece, turned, 0)

    for w in range(windows):
        same[w], cross[w] = grams(grp, w)
    for step in range(1, n_grp):
        for w in range(windows):
            for way in range(2):

                @pl.when(receives(way, step))
                def _():
                    arrival(way, step, w).wait_recv()

                if step < n_grp - 1:

                    @pl.when(sends(way, step + 1))
                    def _():
                        hop(way, step + 1, w).start()

            for way in range(2):

                @pl.when(receives(way, step))
                def _():
                    source = grp - step if way == 0 else grp + step
                    more_same, more_cross = grams(source, w)
                    same[w] += more_same
                    cross[w] += more_cross

    for w in range(windows):
        same[w] = jnp.where(col >= row, same[w], cross[w])

    def mixed(shares, u):
        total = same[0] * shares[u, 0:1, :]
        for w in range(1, windows):
            total = total + same[w] * shares[u, w : w + 1, :]
        return total

    side = lax.rem(beam, 2)
    chip = lax.div(beam, 2)
    chips = n_beam // 2
    p_copies = [
        pltpu.make_async_remote_copy(
            src_ref=passing.at[i],
            dst_ref=passed.at[i],
            send_sem=p_send.at[i],
            recv_sem=p_recv.at[i],
            device_id=(beam + 1 - 2 * side, grp),
            device_id_type=MESH,
        )
        for i in range(chips)
    ]
    o_copies = [
        pltpu.make_async_remote_copy(
            src_ref=outgoing.at[i - 1],
            dst_ref=incoming.at[i - 1],
            send_sem=o_send.at[i - 1],
            recv_sem=o_recv.at[i - 1],
            device_id=(2 * lax.rem(chip + chips - i, chips) + side, grp),
            device_id_type=MESH,
        )
        for i in range(1, chips)
    ]
    for copy in w_copies:
        copy.wait_recv()
    order = list(range(1, chips)) + [0]
    for at, i in enumerate(order):
        shares = weights_in[lax.rem(2 * i + 2 * side + n_beam - 1, n_beam) - 1]
        for u in range(users):
            passing[i, u] = mixed(shares, u)
        if at > 0:
            p_copies[order[at - 1]].start()
    for i in range(1, chips):
        for u in range(users):
            outgoing[i - 1, u] = mixed(weights_in[2 * i - 1], u)
        if i == 1:
            p_copies[order[-1]].start()
    for u in range(users):
        out_ref[u] = mixed(weights[beam], u)
    if chips == 1:
        p_copies[0].start()
    for i in range(1, chips):
        p_copies[i].wait_recv()
        for u in range(users):
            outgoing[i - 1, u] += passed[i, u]
        if i > 1:
            o_copies[i - 2].start()
    p_copies[0].wait_recv()
    for u in range(users):
        out_ref[u] += passed[0, u]
    if chips > 1:
        o_copies[-1].start()

    points = grid_ref.shape[-1]
    chunk = math.gcd(CHUNK, points)
    beam_at = lax.broadcasted_iota(jnp.int32, (width, chunk), 0) * OVERSAMPLE
    for u in range(users):

        @pl.loop(0, points // chunk)
        def _(at):
            span = pl.ds(pl.multiple_of(at * chunk, chunk), chunk)
            offset = (grid_ref[u, :, span] - beam_at).astype(jnp.float32) + 0.5
            angle = offset * (math.pi / (OVERSAMPLE * beams_total))
            sq = angle * angle
            sine = offset * (
                1.0 + sq * (-1.0 / 6 + sq * (1.0 / 120 + sq * (-1.0 / 5040 + sq * (1.0 / 362880))))
            )
            steer = OVERSAMPLE / sine
            high_made[u, :, span], low_made[u, :, span] = halves(steer)
            norm_ref[u, :, span] = jnp.sum(steer * steer, axis=0, keepdims=True)

    stored = [
        pltpu.make_async_copy(high_made, high_ref, store_sem.at[0]),
        pltpu.make_async_copy(low_made, low_ref, store_sem.at[1]),
    ]
    for copy in stored:
        copy.start()
    for i in range(1, chips):
        o_copies[i - 1].wait_recv()
        for u in range(users):
            out_ref[u] += incoming[i - 1, u]
    for copy in w_copies + p_copies + o_copies:
        copy.wait_send()
    for copy in stored:
        copy.wait()
    for way in range(2):
        for step in range(1, n_grp):

            @pl.when(sends(way, step))
            def _():
                for w in range(windows):
                    hop(way, step, w).wait_send()


def exchange(beam_data, counts, owners, slot_window, grid_index, n_beam, n_grp):
    rows = beam_data.shape[2]
    windows = rows // WIN_BEAMS
    padded = -(-windows // 8) * 8
    users, points = grid_index.shape[0], grid_index.shape[2]
    width = WIN_BEAMS
    sums = (users, width, width)
    shares = (users, padded, width)
    vmem = pl.BlockSpec(memory_space=pltpu.VMEM)
    smem = pl.BlockSpec(memory_space=pltpu.SMEM)
    anywhere = pl.BlockSpec(memory_space=pl.ANY)
    return pl.pallas_call(
        functools.partial(exchange_kernel, n_beam, n_grp, windows, rows * n_beam),
        out_shape=[
            jax.ShapeDtypeStruct(sums, jnp.float32),
            jax.ShapeDtypeStruct((users, width, points), jnp.bfloat16),
            jax.ShapeDtypeStruct((users, width, points), jnp.bfloat16),
            jax.ShapeDtypeStruct((users, 1, points), jnp.float32),
        ],
        in_specs=[vmem, smem, smem, smem, vmem],
        out_specs=[vmem, anywhere, anywhere, vmem],
        scratch_shapes=[
            pltpu.VMEM((n_grp, windows, 2 * beam_data.shape[1], width), jnp.bfloat16),
            pltpu.VMEM((n_beam,) + shares, jnp.float32),
            pltpu.VMEM((n_beam - 1,) + shares, jnp.float32),
            pltpu.VMEM((n_beam // 2,) + sums, jnp.float32),
            pltpu.VMEM((n_beam // 2,) + sums, jnp.float32),
            pltpu.VMEM((n_beam // 2 - 1,) + sums, jnp.float32),
            pltpu.VMEM((n_beam // 2 - 1,) + sums, jnp.float32),
            pltpu.VMEM((windows, width, width), jnp.float32),
            pltpu.VMEM((windows, width, width), jnp.float32),
            pltpu.VMEM((users, width, points), jnp.bfloat16),
            pltpu.VMEM((users, width, points), jnp.bfloat16),
            pltpu.SemaphoreType.DMA((2,)),
            pltpu.SemaphoreType.DMA((2, n_grp - 1, windows)),
            pltpu.SemaphoreType.DMA((2, n_grp - 1, windows)),
            pltpu.SemaphoreType.DMA((n_beam - 1,)),
            pltpu.SemaphoreType.DMA((n_beam - 1,)),
            pltpu.SemaphoreType.DMA((n_beam // 2,)),
            pltpu.SemaphoreType.DMA((n_beam // 2,)),
            pltpu.SemaphoreType.DMA((n_beam // 2 - 1,)),
            pltpu.SemaphoreType.DMA((n_beam // 2 - 1,)),
        ],
        compiler_params=pltpu.CompilerParams(collective_id=0, has_side_effects=True),
    )(beam_data, counts, owners, slot_window, grid_index)


def spectrum_kernel(
    beams_total, sum_ref, count_ref, high_ref, low_ref, norm_ref, out_ref, basis_ref, high, low, load_sem
):
    user = pl.program_id(0)
    loads = [
        pltpu.make_async_copy(high_ref.at[user], high, load_sem.at[0]),
        pltpu.make_async_copy(low_ref.at[user], low, load_sem.at[1]),
    ]
    for copy in loads:
        copy.start()
    width, dim = WIN_BEAMS, NOISE_DIM
    packed = sum_ref[0]
    flipped = packed.T
    row = lax.broadcasted_iota(jnp.int32, (width, width), 0)
    col = lax.broadcasted_iota(jnp.int32, (width, width), 1)
    count = count_ref[user].astype(jnp.float32)
    inverse_count = 1.0 / (jnp.zeros((1, width), jnp.float32) + count * SNAPS)
    real_sum = jnp.where(col >= row, packed, flipped) * inverse_count
    imag_sum = jnp.where(col < row, packed, jnp.where(col > row, -flipped, 0.0)) * inverse_count
    covariance = jnp.concatenate(
        [
            jnp.concatenate([real_sum, -imag_sum], axis=1),
            jnp.concatenate([imag_sum, real_sum], axis=1),
        ],
        axis=0,
    )
    parts = halves(covariance)
    squared = dot3(parts, parts)
    square = halves(squared)
    fourth = dot3(square, [half[:, :width] for half in square])
    energy = 2.0 * jnp.sum(fourth * fourth, keepdims=True)
    shift_value = shift_factor * jnp.sqrt(jnp.sqrt(jnp.sqrt(energy)))
    row2 = lax.broadcasted_iota(jnp.int32, (2 * width, 2 * width), 0)
    col2 = lax.broadcasted_iota(jnp.int32, (2 * width, 2 * width), 1)
    eye2 = jnp.where(row2 == col2, 1.0, 0.0)
    by_shift = 1.0 / shift_value
    reduced = covariance * by_shift
    shifted = eye2 - reduced

    def chosen(matrix):
        return jnp.concatenate([matrix[:, :dim], matrix[:, width : width + dim]], axis=1)

    eye = jnp.where(row == col, 1.0, 0.0)

    def cubic(block, pairs):
        for a, b in pairs:
            gram = dot_tn(block, block)
            block = dot(block, a * eye - b * gram)
        return block

    second = halves((shifted - reduced) + squared * by_shift * by_shift)
    power = dot3(second, second)
    block = dot3(halves(power), halves(chosen(power)))
    parts = halves(block)
    gram = dot3(parts, parts, 0)
    scale = 2.0**0.25 * lax.rsqrt(jnp.sqrt(jnp.sum(gram * gram, keepdims=True)))
    block, gram = block * scale, gram * (scale * scale)
    for step, (a, b) in enumerate(cubic_schedule(FAST_LOW, FAST_STEPS)):
        parts = halves(block)
        if step >= FAST_COARSE:
            gram = dot3(parts, parts, 0)
        elif step > 0:
            gram = plain(parts[0], parts[0], 0)
        block = a * block - b * dot3(parts, halves(gram))
    miss = gram - eye
    well = jnp.sum(miss * miss) < FAST_MISS

    def put(basis):
        theta = row.astype(jnp.float32) * (math.pi / beams_total)
        weight = basis[:width] * jnp.cos(theta) + basis[width:] * jnp.sin(theta)
        weight = halves(weight.T)
        points = norm_ref.shape[-1]
        chunk = math.gcd(CHUNK, points)
        for at in range(0, points, chunk):
            span = slice(at, at + chunk)
            projected = dot3(weight, (high[:, span], low[:, span]))
            leakage = jnp.sum(projected * projected, axis=0, keepdims=True) / norm_ref[0, :, span]
            out_ref[0, :, span] = 1.0 / (leakage + spectral_floor)

    for copy in loads:
        copy.wait()
    put(block)

    @pl.when(jnp.logical_not(well))
    def _():
        start = jnp.where(
            (row2 == col2)[:, :width] & (col < dim)[:1], 1.0, 0.0
        ) + jnp.where(row2[:, :width] == col2[:, :width] + (width - dim), 1.0, 0.0) * jnp.where(
            col2[:, :width] >= dim, 1.0, 0.0
        )
        basis_ref[...] = start
        second = dot(shifted, shifted)
        pairs = cubic_schedule(0.0132, 5)

        @pl.loop(0, ITERS // 2)
        def _(_):
            basis_ref[...] = cubic(dot(second, basis_ref[...]), pairs)

        basis_ref[...] = cubic(basis_ref[...], [(1.5, 0.5)] * 4)
        put(basis_ref[...])


def finish_users(sums, counts, high, low, norm, beams_total):
    users, width, points = high.shape

    def block(*shape):
        return pl.BlockSpec((1,) + shape, lambda u: (u, 0, 0))

    return pl.pallas_call(
        functools.partial(spectrum_kernel, beams_total),
        grid=(users,),
        out_shape=jax.ShapeDtypeStruct((users, 1, points), jnp.float32),
        in_specs=[
            block(width, width),
            pl.BlockSpec(memory_space=pltpu.SMEM),
            pl.BlockSpec(memory_space=pl.ANY),
            pl.BlockSpec(memory_space=pl.ANY),
            block(1, points),
        ],
        out_specs=block(1, points),
        scratch_shapes=[
            pltpu.VMEM((2 * width, 2 * NOISE_DIM), jnp.float32),
            pltpu.VMEM((width, points), jnp.bfloat16),
            pltpu.VMEM((width, points), jnp.bfloat16),
            pltpu.SemaphoreType.DMA((2,)),
        ],
    )(sums, counts, high, low, norm).reshape(users, points)


def local(n_beam, n_grp, beam_data, window_count, slot_owner, slot_window, grid_index):
    users, points = grid_index.shape
    sums, high, low, norm = exchange(
        jnp.swapaxes(beam_data, 1, 2),
        window_count,
        slot_owner[:, :, 0],
        slot_window,
        grid_index.reshape(users, 1, points),
        n_beam,
        n_grp,
    )
    return finish_users(
        sums, window_count, high, low, norm, beam_data.shape[1] * n_beam
    )


def solution(mesh):
    placed = (
        P(None, "beam", "grp"),
        P(("beam", "grp")),
        P(("beam", "grp"), None, None),
        P(("beam", "grp"), None),
        P(("beam", "grp"), None),
    )
    return jax.shard_map(
        functools.partial(local, mesh.shape["beam"], mesh.shape["grp"]),
        mesh=mesh,
        in_specs=placed,
        out_specs=P(("beam", "grp"), None),
        check_vma=False,
    )
```

```python
import functools
import math

import jax
import jax.numpy as jnp
from jax import lax
from jax.experimental import pallas as pl
from jax.experimental.pallas import tpu as pltpu
from jax.sharding import PartitionSpec as P

WIN_BEAMS = 128
NOISE_DIM = 64
SNAPS = 256
OVERSAMPLE = 32
ITERS = 8

MESH = pl.DeviceIdType.MESH
highest = lax.Precision.HIGHEST
shift_factor = 1.05
spectral_floor = 0.05
CHUNK = 512
FAST_LOW = 1.0 / 36
FAST_STEPS = 7
FAST_COARSE = 4
FAST_MISS = 2e-4


def cubic_schedule(low, steps):
    pairs = []
    for _ in range(steps):
        form = 1.0 + low + low * low
        scale = 3.0 * math.sqrt(3.0) / (2.0 * form**1.5)
        pairs.append((form * scale, scale))
        low = min((low + low * low) * scale, 1.0)
    return pairs


def dot(left, right):
    return jnp.dot(left, right, precision=highest, preferred_element_type=jnp.float32)


def dot_tn(left, right):
    return lax.dot_general(
        left,
        right,
        (((0,), (0,)), ((), ())),
        precision=highest,
        preferred_element_type=jnp.float32,
    )


def halves(matrix):
    high = matrix.astype(jnp.bfloat16)
    return high, (matrix - high.astype(jnp.float32)).astype(jnp.bfloat16)


def plain(left, right, contract=1):
    return lax.dot_general(
        left,
        right,
        (((contract,), (0,)), ((), ())),
        preferred_element_type=jnp.float32,
    )


def dot3(left, right, contract=1):
    (left_high, left_low), (right_high, right_low) = left, right
    if contract == 1 and left_high.shape[1] <= 128:
        both = plain(
            jnp.concatenate([left_high, left_low], axis=1),
            jnp.concatenate([right_high, right_high], axis=0),
        )
        return both + plain(left_high, right_low)
    return plain(left_high, right_high, contract) + (
        plain(left_high, right_low, contract) + plain(left_low, right_high, contract)
    )


def dot_nt(left, right):
    return lax.dot_general(
        left, right, (((1,), (1,)), ((), ())), preferred_element_type=jnp.float32
    )


def exchange_kernel(
    n_beam,
    n_grp,
    windows,
    beams_total,
    data_ref,
    count_ref,
    owner_ref,
    window_ref,
    grid_ref,
    out_ref,
    high_ref,
    low_ref,
    norm_ref,
    held,
    weights,
    weights_in,
    passing,
    passed,
    outgoing,
    incoming,
    same,
    cross,
    high_made,
    low_made,
    store_sem,
    x_send,
    x_recv,
    w_send,
    w_recv,
    p_send,
    p_recv,
    o_send,
    o_recv,
):
    beam = lax.axis_index("beam")
    grp = lax.axis_index("grp")
    width = WIN_BEAMS
    users, slots = window_ref.shape
    padded = weights.shape[2]

    barrier = pltpu.get_barrier_semaphore()
    has_right = grp < n_grp - 1
    has_left = grp > 0

    @pl.when(has_right)
    def _():
        pl.semaphore_signal(barrier, inc=1, device_id=(beam, grp + 1), device_id_type=MESH)

    @pl.when(has_left)
    def _():
        pl.semaphore_signal(barrier, inc=1, device_id=(beam, grp - 1), device_id_type=MESH)

    for j in range(1, n_beam):
        pl.semaphore_signal(
            barrier, inc=1, device_id=(lax.rem(beam + j, n_beam), grp), device_id_type=MESH
        )

    for w in range(windows):
        columns = slice(w * width, (w + 1) * width)
        held[grp, w] = jnp.concatenate([data_ref[0, :, columns], data_ref[1, :, columns]], axis=0)
    entry = lax.broadcasted_iota(jnp.int32, (n_beam, padded, width), 0) * padded + (
        lax.broadcasted_iota(jnp.int32, (n_beam, padded, width), 1)
    )
    for u in range(users):
        total = jnp.zeros((n_beam, padded, width), jnp.float32)
        for k in range(slots):
            named = owner_ref[u, k] * padded + window_ref[u, k]
            live = (k < count_ref[u]).astype(jnp.float32)
            total = total + jnp.where(entry == named, 1.0, 0.0) * live
        weights[:, u] = total

    pl.semaphore_wait(
        barrier, has_right.astype(jnp.int32) + has_left.astype(jnp.int32) + n_beam - 1
    )

    def hop(way, step, w):
        source = grp - (step - 1) if way == 0 else grp + (step - 1)
        return pltpu.make_async_remote_copy(
            src_ref=held.at[source, w],
            dst_ref=held.at[source, w],
            send_sem=x_send.at[way, step - 1, w],
            recv_sem=x_recv.at[way, step - 1, w],
            device_id=(beam, grp + 1 if way == 0 else grp - 1),
            device_id_type=MESH,
        )

    def arrival(way, step, w):
        source = grp - step if way == 0 else grp + step
        return pltpu.make_async_remote_copy(
            src_ref=held.at[source, w],
            dst_ref=held.at[source, w],
            send_sem=x_send.at[way, step - 1, w],
            recv_sem=x_recv.at[way, step - 1, w],
            device_id=(beam, grp - 1 if way == 0 else grp + 1),
            device_id_type=MESH,
        )

    def sends(way, step):
        if way == 0:
            return has_right & (grp >= step - 1)
        return has_left & (grp + step - 1 < n_grp)

    def receives(way, step):
        return grp >= step if way == 0 else grp + step < n_grp

    for way in range(2):

        @pl.when(sends(way, 1))
        def _():
            for w in range(windows):
                hop(way, 1, w).start()

    w_copies = []
    for j in range(1, n_beam):
        owner = lax.rem(beam + j, n_beam)
        copy = pltpu.make_async_remote_copy(
            src_ref=weights.at[owner],
            dst_ref=weights_in.at[j - 1],
            send_sem=w_send.at[j - 1],
            recv_sem=w_recv.at[j - 1],
            device_id=(owner, grp),
            device_id_type=MESH,
        )
        copy.start()
        w_copies.append(copy)

    row = lax.broadcasted_iota(jnp.int32, (width, width), 0)
    col = lax.broadcasted_iota(jnp.int32, (width, width), 1)
    half = held.shape[2] // 2

    def grams(source, w):
        piece = held[source, w]
        turned = jnp.concatenate([-piece[half:], piece[:half]], axis=0)
        return plain(piece, piece, 0), plain(piece, turned, 0)

    for w in range(windows):
        same[w], cross[w] = grams(grp, w)
    for step in range(1, n_grp):
        for w in range(windows):
            for way in range(2):

                @pl.when(receives(way, step))
                def _():
                    arrival(way, step, w).wait_recv()

                if step < n_grp - 1:

                    @pl.when(sends(way, step + 1))
                    def _():
                        hop(way, step + 1, w).start()

            for way in range(2):

                @pl.when(receives(way, step))
                def _():
                    source = grp - step if way == 0 else grp + step
                    more_same, more_cross = grams(source, w)
                    same[w] += more_same
                    cross[w] += more_cross

    for w in range(windows):
        same[w] = jnp.where(col >= row, same[w], cross[w])

    def mixed(shares, u):
        total = same[0] * shares[u, 0:1, :]
        for w in range(1, windows):
            total = total + same[w] * shares[u, w : w + 1, :]
        return total

    side = lax.rem(beam, 2)
    chip = lax.div(beam, 2)
    chips = n_beam // 2
    p_copies = [
        pltpu.make_async_remote_copy(
            src_ref=passing.at[i],
            dst_ref=passed.at[i],
            send_sem=p_send.at[i],
            recv_sem=p_recv.at[i],
            device_id=(beam + 1 - 2 * side, grp),
            device_id_type=MESH,
        )
        for i in range(chips)
    ]
    o_copies = [
        pltpu.make_async_remote_copy(
            src_ref=outgoing.at[i - 1],
            dst_ref=incoming.at[i - 1],
            send_sem=o_send.at[i - 1],
            recv_sem=o_recv.at[i - 1],
            device_id=(2 * lax.rem(chip + chips - i, chips) + side, grp),
            device_id_type=MESH,
        )
        for i in range(1, chips)
    ]
    for copy in w_copies:
        copy.wait_recv()
    order = list(range(1, chips)) + [0]
    for at, i in enumerate(order):
        shares = weights_in[lax.rem(2 * i + 2 * side + n_beam - 1, n_beam) - 1]
        for u in range(users):
            passing[i, u] = mixed(shares, u)
        if at > 0:
            p_copies[order[at - 1]].start()
    for i in range(1, chips):
        for u in range(users):
            outgoing[i - 1, u] = mixed(weights_in[2 * i - 1], u)
        if i == 1:
            p_copies[order[-1]].start()
    for u in range(users):
        out_ref[u] = mixed(weights[beam], u)
    if chips == 1:
        p_copies[0].start()
    for i in range(1, chips):
        p_copies[i].wait_recv()
        for u in range(users):
            outgoing[i - 1, u] += passed[i, u]
        if i > 1:
            o_copies[i - 2].start()
    p_copies[0].wait_recv()
    for u in range(users):
        out_ref[u] += passed[0, u]
    if chips > 1:
        o_copies[-1].start()

    points = grid_ref.shape[-1]
    chunk = math.gcd(CHUNK, points)
    beam_at = lax.broadcasted_iota(jnp.int32, (width, chunk), 0) * OVERSAMPLE
    for u in range(users):

        @pl.loop(0, points // chunk)
        def _(at):
            span = pl.ds(pl.multiple_of(at * chunk, chunk), chunk)
            offset = (grid_ref[u, :, span] - beam_at).astype(jnp.float32) + 0.5
            angle = offset * (math.pi / (OVERSAMPLE * beams_total))
            sq = angle * angle
            sine = offset * (
                1.0 + sq * (-1.0 / 6 + sq * (1.0 / 120 + sq * (-1.0 / 5040 + sq * (1.0 / 362880))))
            )
            steer = OVERSAMPLE / sine
            high_made[u, :, span], low_made[u, :, span] = halves(steer)
            norm_ref[u, :, span] = jnp.sum(steer * steer, axis=0, keepdims=True)

    stored = [
        pltpu.make_async_copy(high_made, high_ref, store_sem.at[0]),
        pltpu.make_async_copy(low_made, low_ref, store_sem.at[1]),
    ]
    for copy in stored:
        copy.start()
    for i in range(1, chips):
        o_copies[i - 1].wait_recv()
        for u in range(users):
            out_ref[u] += incoming[i - 1, u]
    for copy in w_copies + p_copies + o_copies:
        copy.wait_send()
    for copy in stored:
        copy.wait()
    for way in range(2):
        for step in range(1, n_grp):

            @pl.when(sends(way, step))
            def _():
                for w in range(windows):
                    hop(way, step, w).wait_send()


def exchange(beam_data, counts, owners, slot_window, grid_index, n_beam, n_grp):
    rows = beam_data.shape[2]
    windows = rows // WIN_BEAMS
    padded = -(-windows // 8) * 8
    users, points = grid_index.shape[0], grid_index.shape[2]
    width = WIN_BEAMS
    sums = (users, width, width)
    shares = (users, padded, width)
    vmem = pl.BlockSpec(memory_space=pltpu.VMEM)
    smem = pl.BlockSpec(memory_space=pltpu.SMEM)
    anywhere = pl.BlockSpec(memory_space=pl.ANY)
    return pl.pallas_call(
        functools.partial(exchange_kernel, n_beam, n_grp, windows, rows * n_beam),
        out_shape=[
            jax.ShapeDtypeStruct(sums, jnp.float32),
            jax.ShapeDtypeStruct((users, width, points), jnp.bfloat16),
            jax.ShapeDtypeStruct((users, width, points), jnp.bfloat16),
            jax.ShapeDtypeStruct((users, 1, points), jnp.float32),
        ],
        in_specs=[vmem, smem, smem, smem, vmem],
        out_specs=[vmem, anywhere, anywhere, vmem],
        scratch_shapes=[
            pltpu.VMEM((n_grp, windows, 2 * beam_data.shape[1], width), jnp.bfloat16),
            pltpu.VMEM((n_beam,) + shares, jnp.float32),
            pltpu.VMEM((n_beam - 1,) + shares, jnp.float32),
            pltpu.VMEM((n_beam // 2,) + sums, jnp.float32),
            pltpu.VMEM((n_beam // 2,) + sums, jnp.float32),
            pltpu.VMEM((n_beam // 2 - 1,) + sums, jnp.float32),
            pltpu.VMEM((n_beam // 2 - 1,) + sums, jnp.float32),
            pltpu.VMEM((windows, width, width), jnp.float32),
            pltpu.VMEM((windows, width, width), jnp.float32),
            pltpu.VMEM((users, width, points), jnp.bfloat16),
            pltpu.VMEM((users, width, points), jnp.bfloat16),
            pltpu.SemaphoreType.DMA((2,)),
            pltpu.SemaphoreType.DMA((2, n_grp - 1, windows)),
            pltpu.SemaphoreType.DMA((2, n_grp - 1, windows)),
            pltpu.SemaphoreType.DMA((n_beam - 1,)),
            pltpu.SemaphoreType.DMA((n_beam - 1,)),
            pltpu.SemaphoreType.DMA((n_beam // 2,)),
            pltpu.SemaphoreType.DMA((n_beam // 2,)),
            pltpu.SemaphoreType.DMA((n_beam // 2 - 1,)),
            pltpu.SemaphoreType.DMA((n_beam // 2 - 1,)),
        ],
        compiler_params=pltpu.CompilerParams(collective_id=0, has_side_effects=True),
    )(beam_data, counts, owners, slot_window, grid_index)


def spectrum_kernel(
    beams_total, sum_ref, count_ref, high_ref, low_ref, norm_ref, out_ref, basis_ref, high, low, load_sem
):
    user = pl.program_id(0)
    loads = [
        pltpu.make_async_copy(high_ref.at[user], high, load_sem.at[0]),
        pltpu.make_async_copy(low_ref.at[user], low, load_sem.at[1]),
    ]
    for copy in loads:
        copy.start()
    width, dim = WIN_BEAMS, NOISE_DIM
    packed = sum_ref[0]
    flipped = packed.T
    row = lax.broadcasted_iota(jnp.int32, (width, width), 0)
    col = lax.broadcasted_iota(jnp.int32, (width, width), 1)
    count = count_ref[user].astype(jnp.float32)
    inverse_count = 1.0 / (jnp.zeros((1, width), jnp.float32) + count * SNAPS)
    real_sum = jnp.where(col >= row, packed, flipped) * inverse_count
    imag_sum = jnp.where(col < row, packed, jnp.where(col > row, -flipped, 0.0)) * inverse_count
    covariance = jnp.concatenate(
        [
            jnp.concatenate([real_sum, -imag_sum], axis=1),
            jnp.concatenate([imag_sum, real_sum], axis=1),
        ],
        axis=0,
    )
    parts = halves(covariance)
    squared = dot3(parts, parts)
    square = halves(squared)
    fourth = dot3(square, [half[:, :width] for half in square])
    energy = 2.0 * jnp.sum(fourth * fourth, keepdims=True)
    shift_value = shift_factor * jnp.sqrt(jnp.sqrt(jnp.sqrt(energy)))
    row2 = lax.broadcasted_iota(jnp.int32, (2 * width, 2 * width), 0)
    col2 = lax.broadcasted_iota(jnp.int32, (2 * width, 2 * width), 1)
    eye2 = jnp.where(row2 == col2, 1.0, 0.0)
    by_shift = 1.0 / shift_value
    reduced = covariance * by_shift
    shifted = eye2 - reduced

    def chosen(matrix):
        return jnp.concatenate([matrix[:, :dim], matrix[:, width : width + dim]], axis=1)

    eye = jnp.where(row == col, 1.0, 0.0)

    def cubic(block, pairs):
        for a, b in pairs:
            gram = dot_tn(block, block)
            block = dot(block, a * eye - b * gram)
        return block

    second = halves((shifted - reduced) + squared * by_shift * by_shift)
    power = dot3(second, second)
    block = dot3(halves(power), halves(chosen(power)))
    parts = halves(block)
    gram = dot3(parts, parts, 0)
    scale = 2.0**0.25 * lax.rsqrt(jnp.sqrt(jnp.sum(gram * gram, keepdims=True)))
    block, gram = block * scale, gram * (scale * scale)
    pairs = cubic_schedule(FAST_LOW, FAST_STEPS)
    for step, (a, b) in enumerate(pairs[:-1]):
        parts = halves(block)
        if step >= FAST_COARSE:
            gram = dot3(parts, parts, 0)
        elif step > 0:
            gram = plain(parts[0], parts[0], 0)
        block = a * block - b * dot3(parts, halves(gram))
    parts = halves(block)
    gram = dot3(parts, parts, 0)
    miss = gram - eye
    well = jnp.sum(miss * miss) < FAST_MISS

    def folded(basis):
        theta = row.astype(jnp.float32) * (math.pi / beams_total)
        return (basis[:width] * jnp.cos(theta) + basis[width:] * jnp.sin(theta)).T

    def put(weight):
        weight = halves(weight)
        points = norm_ref.shape[-1]
        chunk = math.gcd(CHUNK, points)
        for at in range(0, points, chunk):
            span = slice(at, at + chunk)
            projected = dot3(weight, (high[:, span], low[:, span]))
            leakage = jnp.sum(projected * projected, axis=0, keepdims=True) / norm_ref[0, :, span]
            out_ref[0, :, span] = 1.0 / (leakage + spectral_floor)

    for copy in loads:
        copy.wait()
    last_a, last_b = pairs[-1]
    weight = folded(block)
    put(last_a * weight - last_b * dot3(halves(gram), halves(weight)))

    @pl.when(jnp.logical_not(well))
    def _():
        start = jnp.where(
            (row2 == col2)[:, :width] & (col < dim)[:1], 1.0, 0.0
        ) + jnp.where(row2[:, :width] == col2[:, :width] + (width - dim), 1.0, 0.0) * jnp.where(
            col2[:, :width] >= dim, 1.0, 0.0
        )
        basis_ref[...] = start
        second = dot(shifted, shifted)
        pairs = cubic_schedule(0.0132, 5)

        @pl.loop(0, ITERS // 2)
        def _(_):
            basis_ref[...] = cubic(dot(second, basis_ref[...]), pairs)

        basis_ref[...] = cubic(basis_ref[...], [(1.5, 0.5)] * 4)
        put(folded(basis_ref[...]))


def finish_users(sums, counts, high, low, norm, beams_total):
    users, width, points = high.shape

    def block(*shape):
        return pl.BlockSpec((1,) + shape, lambda u: (u, 0, 0))

    return pl.pallas_call(
        functools.partial(spectrum_kernel, beams_total),
        grid=(users,),
        out_shape=jax.ShapeDtypeStruct((users, 1, points), jnp.float32),
        in_specs=[
            block(width, width),
            pl.BlockSpec(memory_space=pltpu.SMEM),
            pl.BlockSpec(memory_space=pl.ANY),
            pl.BlockSpec(memory_space=pl.ANY),
            block(1, points),
        ],
        out_specs=block(1, points),
        scratch_shapes=[
            pltpu.VMEM((2 * width, 2 * NOISE_DIM), jnp.float32),
            pltpu.VMEM((width, points), jnp.bfloat16),
            pltpu.VMEM((width, points), jnp.bfloat16),
            pltpu.SemaphoreType.DMA((2,)),
        ],
    )(sums, counts, high, low, norm).reshape(users, points)


def local(n_beam, n_grp, beam_data, window_count, slot_owner, slot_window, grid_index):
    users, points = grid_index.shape
    sums, high, low, norm = exchange(
        jnp.swapaxes(beam_data, 1, 2),
        window_count,
        slot_owner[:, :, 0],
        slot_window,
        grid_index.reshape(users, 1, points),
        n_beam,
        n_grp,
    )
    return finish_users(
        sums, window_count, high, low, norm, beam_data.shape[1] * n_beam
    )


def solution(mesh):
    placed = (
        P(None, "beam", "grp"),
        P(("beam", "grp")),
        P(("beam", "grp"), None, None),
        P(("beam", "grp"), None),
        P(("beam", "grp"), None),
    )
    return jax.shard_map(
        functools.partial(local, mesh.shape["beam"], mesh.shape["grp"]),
        mesh=mesh,
        in_specs=placed,
        out_specs=P(("beam", "grp"), None),
        check_vma=False,
    )
```
